128 devices in a mesh: panel: 16 (over z, x), prb: 8 (over y, core).
Axes of the slice: x: 4, y: 4, z: 4, core: 2. Of those that a mesh axis runs over, the one named last changes fastest.
Arguments:
- channel: bfloat16 [224, 256, 64, 128], P('panel', 'prb'), may hold values from -0.125 to 0.125
- received: bfloat16 [224, 256, 64, 288], P('panel', 'prb'), may hold values from -6 to 6
- keep_list: int32 [224, 256, 3], P('panel', 'prb'), may hold values from 0 to 4, as said below
- alloc: int32 [256, 64], replicated, may hold values from 0 to 511, all different within a row
- noise_var: float32 [512], replicated, may hold values from 0.1 to 1
- owner: int32 [256, 64, 1], replicated, may hold values from 0 to 127; in each aligned block of 128 rows (0 to 127, 128 to 255, ..., all dimensions but the last counted through in order) at most 2 rows name the same one
Outputs:
- equalized: float32 [32768, 288], P(('panel', 'prb'))
The draws below stay inside these ranges and needn't reach their ends.
Inputs may be any that keep to these rules, and one draw needn't show every extreme that they name: `keep_list`: entries below 4 name distinct beam blocks of the panel; entries equal to 4 are empty slots and stand after the kept ones; each panel keeps between 1 and 3 blocks for each PRB. `alloc`: each PRB lists 64 different users, and every user is listed by some PRB. Owners are device numbers along panel+prb. In each aligned block of 128 rows (PRB-major, then layer), no owner appears more than 2 times.
All inputs are finite; a program needn't handle non-finite values.
Results may differ from the reference program's by a relative error of at most 0.005.
Values may be sent and summed in bfloat16 or wider, within the bound.
No kernel may reach another device: no remote copies, remote signals or barrier semaphores. Data moves between devices by JAX's collectives and lax.ppermute only.
A program may use at most 192 MiB of HBM per device.

```python
import math
import jax
import jax.numpy as jnp
import numpy as np
from jax import lax

ANTENNA_EDGE = 8
PANEL_ANTENNAS = 64
NBLK = 4
BB = 16
KMAX = 3
KB = 48
LAYERS_PER_PRB = 64
USERS = 512
RESOURCE_ELEMS = 144
PANEL_TOTAL = 224
PRB_OWN = 2
PRB_DEV = 32
SLOT_PRB_TOTAL = 256
CAP = 2
N_PRB = 8
DEVICES = 128


def draw_keep_list(key, part):
    base = jax.random.fold_in(key, 11)
    first_key, second_key = jax.random.split(base)
    scores = jax.random.randint(first_key, (PANEL_TOTAL, SLOT_PRB_TOTAL, NBLK), 0, 1 << 20) * NBLK + jnp.arange(NBLK, dtype=jnp.int32)
    ordered = jnp.argsort(scores, axis=-1, stable=True)[..., :KMAX].astype(jnp.int32)
    counts = jax.random.randint(second_key, (PANEL_TOTAL, SLOT_PRB_TOTAL, 1), 1, KMAX + 1)
    return jnp.where(jnp.arange(KMAX, dtype=jnp.int32)[None, None, :] < counts, ordered, NBLK).astype(jnp.int32)


def block_scale(key, extent, cuts, low, largest):
    def one(dim, shards_of):
        steps = jax.random.uniform(jax.random.fold_in(jax.random.fold_in(key, 6), dim), (shards_of,), jnp.float32, low / len(cuts), largest / len(cuts))
        return jnp.repeat(jnp.exp(steps), extent[dim] // shards_of).reshape((-1,) + (1,) * (len(extent) - dim - 1))

    gain = one(*cuts[0])
    for cut in cuts[1:]:
        gain = gain * one(*cut)
    return gain


def distinct(key, rows, number_of, top, lift):
    ranking = jax.random.permutation(jax.random.fold_in(key, 1), number_of)
    boost = ranking
    for power in range(3):
        boost = boost * boost // number_of
    boost = boost * lift // number_of
    lots = jax.random.randint(jax.random.fold_in(key, 2), (rows, number_of), 0, 4096) + boost
    sure = jax.random.permutation(jax.random.fold_in(key, 3), rows)[jnp.arange(number_of) % rows]
    lots = jnp.where(jnp.arange(rows)[:, None] == sure[None, :], 1 << 14, lots)
    merit = lots * number_of + jnp.arange(number_of)
    return lax.top_k(merit.astype(jnp.int32), top)[1].astype(jnp.int32)


def deal_out(key, own, number, rows, amount, top, limit, slope):
    sequence = jax.random.permutation(key, amount)
    crowded, ordinary = shares(amount, rows * top, limit, slope, True), shares(amount, rows * top, limit, slope, False)
    places = jnp.arange(amount)

    def named(tallies, rotation):
        used = int((tallies > 0).sum())
        fixed = max(1, used // 4)
        passed = fixed + (places - fixed + rotation * (used - fixed)) % max(1, amount - fixed)
        return jnp.zeros((amount,), jnp.int32).at[sequence[jnp.where(places < fixed, places, passed)]].set(jnp.asarray(tallies, jnp.int32))

    tallies = jnp.where(number % 4 == 0, named(crowded, number // 4), named(ordinary, number - number // 4 - 1))
    mixed = jax.random.permutation(jax.random.fold_in(own, 3), amount)
    source_of, receiver = mixed[0:amount // 2 * 2:2], mixed[1:amount // 2 * 2:2]
    slack = jnp.minimum(tallies[source_of] - 1, limit - tallies[receiver]) // 2
    slack = jnp.where((source_of == sequence[0]) | (receiver == sequence[0]) | (tallies[receiver] == 0), 0, jnp.maximum(slack, 0))
    passed = jax.random.randint(jax.random.fold_in(own, 4), (amount // 2,), 0, 1 << 20) % (slack + 1)
    tallies = tallies.at[source_of].add(-passed).at[receiver].add(passed)
    members = jnp.searchsorted(jnp.cumsum(tallies), jnp.arange(rows * top), side="right").astype(jnp.int32)
    listing = members.reshape(top, rows).T
    listing = listing[jax.random.permutation(jax.random.fold_in(own, 1), rows)]
    rotation = jax.random.randint(jax.random.fold_in(own, 2), (rows, 1), 0, top)
    return jnp.take_along_axis(listing, (jnp.arange(top)[None, :] + rotation) % top, axis=1)


def shares(count, total, bound, lean, full):
    loads = [(1 << 20) // math.isqrt(grade ** lean) + 1 for grade in range(1, count + 1)]
    largest = bound if full else min(bound, max(-(-total // count), total * loads[0] // sum(loads)))
    least = 1 if total - largest >= count - 1 else 0
    holding, rest = [largest] + [least] * (count - 1), total - largest - least * (count - 1)
    while rest > 0:
        movable = [i for i in range(1, count) if holding[i] < largest] or [i for i in range(1, count) if holding[i] < bound]
        whole, left = sum([loads[i] for i in movable]), rest
        for i in movable:
            extra = min(bound - holding[i], max(1, left * loads[i] // whole), rest)
            holding[i] = holding[i] + extra
            rest = rest - extra
    return np.array(holding)


def bell_draw(own_key, shape, scale, limit, cuts=(), held_as=jnp.bfloat16):
    drawn = jax.random.normal(own_key, shape, jnp.float32) * scale
    if len(cuts) > 0:
        drawn = block_scale(own_key, shape, cuts, -0.22, 0.18) * drawn
    return jnp.clip(drawn, min=-limit, max=limit).astype(held_as)


def setup_inputs(seed: int = 0) -> dict:
    seeds = jax.random.split(jax.random.key(seed), 7)
    channel = bell_draw(seeds[0], (PANEL_TOTAL, SLOT_PRB_TOTAL, PANEL_ANTENNAS, 2 * LAYERS_PER_PRB), ((PANEL_TOTAL * 64) ** -0.5), 0.125, ((0, 16), (1, 8)))
    received = bell_draw(seeds[1], (PANEL_TOTAL, SLOT_PRB_TOTAL, PANEL_ANTENNAS, 2 * RESOURCE_ELEMS), 1.0, 6.0, ((0, 16), (1, 8)))
    keep_list = draw_keep_list(jax.random.fold_in(seeds[6], 71), 0)
    alloc = distinct(seeds[3], SLOT_PRB_TOTAL, USERS, LAYERS_PER_PRB, 0)
    noise_var = jnp.clip(jnp.exp(jax.random.uniform(seeds[4], (USERS,), jnp.float32, math.log(0.1), math.log(1.0))), 0.1, 1.0)
    owner_keys = jax.random.split(jax.random.fold_in(seeds[5], 1), SLOT_PRB_TOTAL * LAYERS_PER_PRB // (PRB_OWN * LAYERS_PER_PRB))
    owner_turns = jax.random.permutation(jax.random.fold_in(seeds[5], 3), SLOT_PRB_TOTAL * LAYERS_PER_PRB // (PRB_OWN * LAYERS_PER_PRB))
    owner = jax.vmap(lambda own, number: deal_out(jax.random.fold_in(seeds[5], 2), own, number, PRB_OWN * LAYERS_PER_PRB, DEVICES, 1, CAP, 2))(owner_keys, owner_turns).reshape((SLOT_PRB_TOTAL, LAYERS_PER_PRB, 1))
    return {"channel": channel, "received": received, "keep_list": keep_list, "alloc": alloc, "noise_var": noise_var, "owner": owner}


def beamspace_tables(panel_side):
    length = panel_side * panel_side
    positions = jnp.arange(length, dtype=jnp.int32)
    first_axis = positions // panel_side
    second_axis = positions % panel_side
    phases = (first_axis[:, None] * first_axis[None, :] + second_axis[:, None] * second_axis[None, :]) % panel_side
    angles = phases.astype(jnp.float32) * (2.0 * math.pi / panel_side)
    real_part = (jnp.cos(angles) / panel_side).astype(jnp.bfloat16)
    imag_part = (-jnp.sin(angles) / panel_side).astype(jnp.bfloat16)
    return (real_part, imag_part)

def combine_parts(first, second, width):
    return jnp.concatenate([first[..., :width] - second[..., width:], second[..., :width] + first[..., width:]], axis=-1).astype(jnp.bfloat16)

def solve_one(factor_one, right_one):
    return jax.scipy.linalg.cho_solve((factor_one, True), right_one)

def solve_layers(products, noise, layer_count, res_count):
    width = layer_count
    block_a = products[:, :width, :width]
    block_b = products[:, :width, width:2 * width]
    block_c = products[:, width:2 * width, :width]
    block_d = products[:, width:2 * width, width:2 * width]
    identity = jnp.eye(width, dtype=jnp.float32)
    gram_real = block_a + block_d + identity[None] * noise[:, :, None]
    gram_imag = block_b - block_c
    system = jnp.concatenate([jnp.concatenate([gram_real, -gram_imag], 2), jnp.concatenate([gram_imag, gram_real], 2)], 1)
    matched = products[:, :, 2 * width:]
    match_real = matched[:, :width, :res_count] + matched[:, width:, res_count:]
    match_imag = matched[:, :width, res_count:] - matched[:, width:, :res_count]
    right_side = jnp.concatenate([match_real, match_imag], 1)
    factor = jnp.linalg.cholesky(system)
    solved = jax.vmap(solve_one)(factor, right_side)
    rows = jnp.concatenate([solved[:, :width], solved[:, width:]], 2)
    return rows.reshape(-1, 2 * res_count)

def reference(channel, received, keep_list, alloc, noise_var, owner):
    beam_table_real, beam_table_imag = beamspace_tables(ANTENNA_EDGE)
    beam_table_real = beam_table_real.astype(jnp.float32)
    beam_table_imag = beam_table_imag.astype(jnp.float32)
    highest = lax.Precision.HIGHEST

    def transform(signal, width):
        first = jnp.einsum('qa,nac->nqc', beam_table_real, signal, precision=highest)
        second = jnp.einsum('qa,nac->nqc', beam_table_imag, signal, precision=highest)
        return combine_parts(first, second, width)

    def per_prb(prb_index):
        channel_prb = lax.dynamic_index_in_dim(channel, prb_index, 1, keepdims=False).astype(jnp.float32)
        signal_prb = lax.dynamic_index_in_dim(received, prb_index, 1, keepdims=False).astype(jnp.float32)
        keep_prb = lax.dynamic_index_in_dim(keep_list, prb_index, 1, keepdims=False)
        beams = jnp.concatenate([transform(channel_prb, LAYERS_PER_PRB), transform(signal_prb, RESOURCE_ELEMS)], axis=-1)
        selector = (keep_prb[:, :, None] == jnp.arange(NBLK, dtype=jnp.int32)[None, None, :]).astype(jnp.float32)
        shaped = beams.astype(jnp.float32).reshape(PANEL_TOTAL, NBLK, BB, beams.shape[-1])
        kept = jnp.einsum('nkb,nbjc->nkjc', selector, shaped, precision=highest).astype(jnp.bfloat16)
        kept_wide = kept.reshape(PANEL_TOTAL, KB, beams.shape[-1]).astype(jnp.float32)
        products = jnp.einsum('nqc,nqd->cd', kept_wide[..., :2 * LAYERS_PER_PRB], kept_wide, precision=highest)
        alloc_row = lax.dynamic_index_in_dim(alloc, prb_index, 0, keepdims=False)
        matches = alloc_row[:, None] == jnp.arange(USERS, dtype=jnp.int32)[None, :]
        noise = jnp.sum(jnp.where(matches, noise_var[None, :], jnp.float32(0.0)), axis=-1)
        return solve_layers(products[None], noise[None], LAYERS_PER_PRB, RESOURCE_ELEMS)
    rows = lax.map(per_prb, jnp.arange(SLOT_PRB_TOTAL, dtype=jnp.int32))
    blocks = SLOT_PRB_TOTAL // PRB_OWN
    block_rows = PRB_OWN * LAYERS_PER_PRB
    rows_blocked = rows.reshape(blocks, block_rows, 2 * RESOURCE_ELEMS)
    owner_blocked = owner.reshape(blocks, block_rows).astype(jnp.int32)
    onehot = (owner_blocked[:, :, None] == jnp.arange(DEVICES, dtype=jnp.int32)[None, None, :]).astype(jnp.int32)
    earlier = jnp.cumsum(onehot, axis=1) - onehot
    slots = jnp.sum(earlier * onehot, axis=2).astype(jnp.int32)
    first_prb = jnp.arange(blocks, dtype=jnp.int32) * PRB_OWN
    source = first_prb % PRB_DEV // PRB_OWN * N_PRB + first_prb // PRB_DEV
    source_rows = jnp.broadcast_to(source[:, None], (blocks, block_rows)).astype(jnp.int32)
    output = jnp.zeros((DEVICES, DEVICES, CAP, 2 * RESOURCE_ELEMS), jnp.float32)
    output = output.at[owner_blocked, source_rows, slots].set(rows_blocked)
    return output.reshape(DEVICES * DEVICES * CAP, 2 * RESOURCE_ELEMS)
```

```python
import jax
import jax.numpy as jnp
import ml_dtypes
import numpy as np
from jax import lax
from jax.experimental import pallas as pl
from jax.experimental.pallas import tpu as pltpu
from jax.sharding import PartitionSpec as P

EDGE = 8
ANT = EDGE * EDGE
NBLK = 4
LAYERS = 64
RES = 144
PACK = 384


def projector_tables():
    pos = np.arange(ANT)
    first, second = pos // EDGE, pos % EDGE
    phase = (first[:, None] * first[None, :] + second[:, None] * second[None, :]) % EDGE
    cos8 = np.array([1.0, np.sqrt(0.5), 0.0, -np.sqrt(0.5), -1.0, -np.sqrt(0.5), 0.0, np.sqrt(0.5)])
    sin8 = np.array([0.0, np.sqrt(0.5), 1.0, np.sqrt(0.5), 0.0, -np.sqrt(0.5), -1.0, -np.sqrt(0.5)])
    real = (cos8[phase] / EDGE).astype(ml_dtypes.bfloat16).astype(np.float64)
    imag = (-sin8[phase] / EDGE).astype(ml_dtypes.bfloat16).astype(np.float64)
    beams = real + 1j * imag
    table = np.zeros((2, 1 << NBLK, ANT, 4 * ANT), np.float64)
    rows = ANT // NBLK
    for pattern in range(1 << NBLK):
        keep = np.array([(pattern >> (q // rows)) & 1 for q in range(ANT)], np.float64)
        proj = np.conj(beams.T) @ (keep[:, None] * beams)
        for half in range(2):
            table[half, pattern, :, half * ANT : (half + 1) * ANT] = proj.real
            table[half, pattern, :, (2 + half) * ANT : (3 + half) * ANT] = proj.imag
    return table.astype(ml_dtypes.bfloat16)


TABLE = projector_tables()


def rotated(m, width):
    return jnp.concatenate([m[:, width:], -m[:, :width]], axis=1)


def sums_kernel(pats_ref, table_ref, ch_ref, rx_ref, out_ref, *, panels, prbs, steps_prb):
    step = pl.program_id(0)
    for j in range(prbs):
        p = step * prbs + j
        pieces = []
        for n in range(0, panels, 2):
            pair = ch_ref[n : n + 2, j].reshape(2 * ANT, 2 * LAYERS)
            weights = jnp.concatenate(
                [
                    table_ref[0, pats_ref[n * steps_prb + p]],
                    table_ref[1, pats_ref[(n + 1) * steps_prb + p]],
                ],
                axis=0,
            )
            ab = jnp.dot(pair.T, weights, preferred_element_type=jnp.float32)
            a, b = ab[:, : 2 * ANT], ab[:, 2 * ANT :]
            pieces.append(
                jnp.concatenate(
                    [a[:LAYERS] + b[LAYERS:], a[LAYERS:] - b[:LAYERS]], axis=0
                ).astype(jnp.bfloat16)
            )
        left = jnp.concatenate(pieces, axis=1)
        ch = ch_ref[:, j].reshape(panels * ANT, 2 * LAYERS)
        rx = rx_ref[:, j].reshape(panels * ANT, 2 * RES)
        head = jnp.dot(left, rx[:, :256], preferred_element_type=jnp.float32)
        rest = jnp.dot(
            left, jnp.concatenate([ch, rx[:, 256:]], axis=1), preferred_element_type=jnp.float32
        )
        my = jnp.concatenate([head, rest[:, 128:]], axis=1)
        mh = rest[:, :128]
        z = my[:LAYERS] + rotated(my[LAYERS:], RES)
        g = mh[:LAYERS] + rotated(mh[LAYERS:], LAYERS)
        swapped = pltpu.roll(g, LAYERS, axis=1)
        row = lax.broadcasted_iota(jnp.int32, (LAYERS, 128), 0)
        lane = lax.broadcasted_iota(jnp.int32, (LAYERS, 128), 1)
        packed = jnp.where(row >= lane - LAYERS, swapped, g)
        out_ref[j, :, :256] = z[:, :256].astype(jnp.bfloat16)
        tail = jnp.concatenate([z[:, 256:], jnp.zeros((LAYERS, 96), jnp.float32)], axis=1)
        out_ref[j, :, 256:] = jnp.where(lane >= LAYERS, packed, tail).astype(jnp.bfloat16)


def panel_sums(pats, channel, received):
    panels, prb_local = channel.shape[:2]
    prbs = 2
    import functools

    kernel = functools.partial(sums_kernel, panels=panels, prbs=prbs, steps_prb=prb_local)
    return pl.pallas_call(
        kernel,
        grid_spec=pltpu.PrefetchScalarGridSpec(
            num_scalar_prefetch=1,
            grid=(prb_local // prbs,),
            in_specs=[
                pl.BlockSpec(TABLE.shape, lambda i, s: (0, 0, 0, 0)),
                pl.BlockSpec((panels, prbs, ANT, 2 * LAYERS), lambda i, s: (0, i, 0, 0)),
                pl.BlockSpec((panels, prbs, ANT, 2 * RES), lambda i, s: (0, i, 0, 0)),
            ],
            out_specs=pl.BlockSpec((prbs, LAYERS, PACK), lambda i, s: (i, 0, 0)),
        ),
        out_shape=jax.ShapeDtypeStruct((prb_local, LAYERS, PACK), jnp.bfloat16),
        compiler_params=pltpu.CompilerParams(dimension_semantics=("arbitrary",)),
        name="panel_sums",
    )(pats, jnp.asarray(TABLE), channel, received)


def solve_kernel(arr_ref, noise_ref, place_ref, out_ref, *, sources):
    def total(j):
        acc = arr_ref[0, j].astype(jnp.float32)
        for s in range(1, sources):
            acc = acc + arr_ref[s, j].astype(jnp.float32)
        return acc

    s0, s1 = total(0), total(1)
    row = lax.broadcasted_iota(jnp.int32, (LAYERS, 128), 0)
    lane = lax.broadcasted_iota(jnp.int32, (LAYERS, 128), 1)
    upper = lane >= LAYERS
    col = jnp.where(upper, lane - LAYERS, lane)
    q = jnp.where(upper, s1[:, 256:], pltpu.roll(s0[:, 256:], LAYERS, axis=1))
    qt = jnp.concatenate([q, jnp.zeros_like(q)], axis=0).T
    qt = jnp.where(upper, pltpu.roll(qt[LAYERS:], LAYERS, axis=1), qt[:LAYERS])
    ar = jnp.where(row >= col, q, qt) + jnp.where(row == col, noise_ref[...], 0.0)
    ai = jnp.where(col > row, q, jnp.where(col < row, -qt, 0.0))
    base = jnp.where(upper, LAYERS, 0)
    for k in range(LAYERS):
        idx = base + k
        cr = jnp.take_along_axis(ar, idx, axis=1, mode="promise_in_bounds")
        ci = jnp.take_along_axis(ai, idx, axis=1, mode="promise_in_bounds")
        inv = 1.0 / cr[k : k + 1]
        here = col == k
        ar = jnp.where(here, 0.0, ar)
        ai = jnp.where(here, 0.0, ai)
        rr = jnp.where(here[:1], inv, ar[k : k + 1] * inv)
        ri = ai[k : k + 1] * inv
        ar = ar - (cr * rr - ci * ri)
        ai = ai - (cr * ri + ci * rr)
        this = row == k
        ar = jnp.where(this, rr, ar)
        ai = jnp.where(this, ri, ai)
    z = jnp.concatenate([s0[:, : 2 * RES], s1[:, : 2 * RES]], axis=0)
    rows = []
    for half in (~upper, upper):
        left = jnp.concatenate([jnp.where(half, ar, 0.0), jnp.where(half, ai, 0.0)], axis=0)
        r = jnp.dot(left, z, precision=lax.Precision.HIGHEST, preferred_element_type=jnp.float32)
        rows.append(r[:LAYERS] - rotated(r[LAYERS:], RES))
    x = jnp.concatenate(rows, axis=0).astype(jnp.bfloat16)
    out_ref[...] = jnp.dot(place_ref[...], x, preferred_element_type=jnp.float32).astype(jnp.bfloat16)


def solve_and_route(arrived, noise, place):
    import functools

    return pl.pallas_call(
        functools.partial(solve_kernel, sources=arrived.shape[0]),
        out_shape=jax.ShapeDtypeStruct((place.shape[0], 2 * RES), jnp.bfloat16),
        name="solve_and_route",
    )(arrived, noise, place)


def body(channel, received, keep_list, alloc, noise_var, owner):
    panel_count = lax.axis_size("panel")
    prb_count = lax.axis_size("prb")
    prb_local = channel.shape[1]
    prb_own = prb_local // panel_count
    pats = jnp.sum(jnp.where(keep_list < NBLK, 1 << keep_list, 0), axis=-1).astype(jnp.int32)
    sums = panel_sums(pats.reshape(-1), channel, received)
    parts = sums.reshape(panel_count, prb_own, LAYERS, PACK)
    arrived = lax.all_to_all(parts, "panel", split_axis=0, concat_axis=0, tiled=True)

    first_prb = lax.axis_index("prb") * prb_local + lax.axis_index("panel") * prb_own
    alloc_rows = lax.dynamic_slice_in_dim(alloc, first_prb, prb_own, 0)
    owner_rows = lax.dynamic_slice_in_dim(owner, first_prb, prb_own, 0).reshape(-1)
    users = jnp.arange(noise_var.shape[0], dtype=jnp.int32)
    matches = alloc_rows[:, :, None] == users[None, None, :]
    noise = jnp.sum(jnp.where(matches, noise_var[None, None, :], jnp.float32(0.0)), axis=-1)
    devices = panel_count * prb_count
    capacity = 2
    total = owner_rows.shape[0]
    same = owner_rows[:, None] == owner_rows[None, :]
    before = jnp.arange(total)[:, None] < jnp.arange(total)[None, :]
    slots = jnp.sum(jnp.where(same & before, 1, 0), axis=0)
    target = owner_rows * capacity + slots
    place = (jnp.arange(devices * capacity)[:, None] == target[None, :]).astype(jnp.bfloat16)

    outgoing = solve_and_route(arrived, noise.reshape(1, -1), place)
    shaped = outgoing.reshape(devices, capacity, 2 * RES)
    final = lax.all_to_all(shaped, ("panel", "prb"), split_axis=0, concat_axis=0, tiled=True)
    return final.reshape(-1, 2 * RES).astype(jnp.float32)


def solution(mesh):
    placed = (
        P("panel", "prb", None, None),
        P("panel", "prb", None, None),
        P("panel", "prb", None),
        P(),
        P(),
        P(),
    )
    return jax.shard_map(
        body, mesh=mesh, in_specs=placed, out_specs=P(("panel", "prb"), None), check_vma=False
    )
```

```python
import functools

import jax
import jax.numpy as jnp
import ml_dtypes
import numpy as np
from jax import lax
from jax.experimental import pallas as pl
from jax.experimental.pallas import tpu as pltpu
from jax.sharding import PartitionSpec as P

EDGE = 8
ANT = EDGE * EDGE
NBLK = 4
LAYERS = 64
RES = 144
PACK = 384


def projector_tables():
    pos = np.arange(ANT)
    first, second = pos // EDGE, pos % EDGE
    phase = (first[:, None] * first[None, :] + second[:, None] * second[None, :]) % EDGE
    cos8 = np.array([1.0, np.sqrt(0.5), 0.0, -np.sqrt(0.5), -1.0, -np.sqrt(0.5), 0.0, np.sqrt(0.5)])
    sin8 = np.array([0.0, np.sqrt(0.5), 1.0, np.sqrt(0.5), 0.0, -np.sqrt(0.5), -1.0, -np.sqrt(0.5)])
    real = (cos8[phase] / EDGE).astype(ml_dtypes.bfloat16).astype(np.float64)
    imag = (-sin8[phase] / EDGE).astype(ml_dtypes.bfloat16).astype(np.float64)
    beams = real + 1j * imag
    table = np.zeros((2, 1 << NBLK, ANT, 4 * ANT), np.float64)
    rows = ANT // NBLK
    for pattern in range(1 << NBLK):
        keep = np.array([(pattern >> (q // rows)) & 1 for q in range(ANT)], np.float64)
        proj = np.conj(beams.T) @ (keep[:, None] * beams)
        for half in range(2):
            table[half, pattern, :, half * ANT : (half + 1) * ANT] = proj.real
            table[half, pattern, :, (2 + half) * ANT : (3 + half) * ANT] = proj.imag
    return table.astype(ml_dtypes.bfloat16)


TABLE = projector_tables()


def rotated(m, width):
    return jnp.concatenate([m[:, width:], -m[:, :width]], axis=1)


def sums_kernel(
    pats_ref, table_hbm, ch_hbm, rx_hbm, out_hbm, table_ref, ch_buf, rx_buf, out_buf, table_sem,
    in_sems, out_sems, *, panels, pieces, prbs,
):
    def incoming(i):
        rows = pl.ds(i * prbs, prbs)
        return (
            pltpu.make_async_copy(ch_hbm.at[:, rows], ch_buf.at[:, rows], in_sems.at[0, i]),
            pltpu.make_async_copy(rx_hbm.at[:, rows], rx_buf.at[:, rows], in_sems.at[1, i]),
        )

    def leaving(i):
        rows = pl.ds(i * prbs, prbs)
        return pltpu.make_async_copy(out_buf.at[rows], out_hbm.at[rows], out_sems.at[i])

    table_copy = pltpu.make_async_copy(table_hbm, table_ref, table_sem)
    for i in range(pieces):
        if i == 0:
            table_copy.start()
        for copy in incoming(i):
            copy.start()
    table_copy.wait()
    row = lax.broadcasted_iota(jnp.int32, (LAYERS, 128), 0)
    lane = lax.broadcasted_iota(jnp.int32, (LAYERS, 128), 1)

    def piece(i, carry):
        for copy in incoming(i):
            copy.wait()
        for j in range(prbs):
            local = i * prbs + j
            pieces_t = []
            for n in range(0, panels, 2):
                pair = ch_buf[n : n + 2, local].reshape(2 * ANT, 2 * LAYERS)
                weights = jnp.concatenate(
                    [
                        table_ref[0, pats_ref[n, local]],
                        table_ref[1, pats_ref[n + 1, local]],
                    ],
                    axis=0,
                )
                ab = jnp.dot(pair.T, weights, preferred_element_type=jnp.float32)
                a, b = ab[:, : 2 * ANT], ab[:, 2 * ANT :]
                pieces_t.append(
                    jnp.concatenate(
                        [a[:LAYERS] + b[LAYERS:], a[LAYERS:] - b[:LAYERS]], axis=0
                    ).astype(jnp.bfloat16)
                )
            left = jnp.concatenate(pieces_t, axis=1)
            ch = ch_buf[:, local].reshape(panels * ANT, 2 * LAYERS)
            rx = rx_buf[:, local].reshape(panels * ANT, 2 * RES)
            head = jnp.dot(left, rx[:, :256], preferred_element_type=jnp.float32)
            rest = jnp.dot(
                left, jnp.concatenate([ch, rx[:, 256:]], axis=1), preferred_element_type=jnp.float32
            )
            my = jnp.concatenate([head, rest[:, 128:]], axis=1)
            mh = rest[:, :128]
            z = my[:LAYERS] + rotated(my[LAYERS:], RES)
            g = mh[:LAYERS] + rotated(mh[LAYERS:], LAYERS)
            swapped = pltpu.roll(g, LAYERS, axis=1)
            packed = jnp.where(row >= lane - LAYERS, swapped, g)
            tail = jnp.concatenate([z[:, 256:], jnp.zeros((LAYERS, 96), jnp.float32)], axis=1)
            out_buf[local, :, :256] = z[:, :256].astype(out_buf.dtype)
            out_buf[local, :, 256:] = jnp.where(lane >= LAYERS, packed, tail).astype(out_buf.dtype)
        leaving(i).start()
        return carry

    lax.fori_loop(0, pieces, piece, 0)
    for i in range(pieces):
        leaving(i).wait()


def panel_sums(pats, channel, received, prbs=4):
    panels, prb_local = channel.shape[:2]
    pieces = prb_local // prbs
    kernel = functools.partial(sums_kernel, panels=panels, pieces=pieces, prbs=prbs)
    return pl.pallas_call(
        kernel,
        grid_spec=pltpu.PrefetchScalarGridSpec(
            num_scalar_prefetch=1,
            grid=(1,),
            in_specs=[pl.BlockSpec(memory_space=pl.ANY)] * 3,
            out_specs=pl.BlockSpec(memory_space=pl.ANY),
            scratch_shapes=[
                pltpu.VMEM(TABLE.shape, jnp.bfloat16),
                pltpu.VMEM((panels, prb_local, ANT, 2 * LAYERS), jnp.bfloat16),
                pltpu.VMEM((panels, prb_local, ANT, 2 * RES), jnp.bfloat16),
                pltpu.VMEM((prb_local, LAYERS, PACK), jnp.bfloat16),
                pltpu.SemaphoreType.DMA(()),
                pltpu.SemaphoreType.DMA((2, pieces)),
                pltpu.SemaphoreType.DMA((pieces,)),
            ],
        ),
        out_shape=jax.ShapeDtypeStruct((prb_local, LAYERS, PACK), jnp.bfloat16),
        compiler_params=pltpu.CompilerParams(dimension_semantics=("arbitrary",)),
        name="panel_sums",
    )(pats, jnp.asarray(TABLE), channel, received)


TILE = 8
GROUP = 4


def less_product(acc, left, right):
    return (
        acc[0] - (left[0] * right[0] - left[1] * right[1]),
        acc[1] - (left[0] * right[1] + left[1] * right[0]),
    )


def inverse_tiles(tiles, col, base):
    count = len(tiles) * TILE
    row = lax.broadcasted_iota(jnp.int32, col.shape, 0)
    for k in range(0, count, GROUP):
        spread = []
        for j in range(GROUP):
            idx = base + (k + j)
            spread.append(
                [
                    tuple(
                        jnp.take_along_axis(part, idx, axis=1, mode="promise_in_bounds")
                        for part in tile
                    )
                    for tile in tiles
                ]
            )
        for j in range(GROUP):
            at = k + j
            t, r = at // TILE, at % TILE
            here = col == at
            this = row == r
            column = spread[j]
            inv = 1.0 / column[t][0][r : r + 1]
            pivot = (
                jnp.where(here[:1], inv, tiles[t][0][r : r + 1] * inv),
                jnp.where(here[:1], 0.0, tiles[t][1][r : r + 1] * inv),
            )
            tiles = [
                less_product(tuple(jnp.where(here, 0.0, part) for part in tile), c, pivot)
                for tile, c in zip(tiles, column)
            ]
            tiles[t] = tuple(jnp.where(this, p, part) for p, part in zip(pivot, tiles[t]))
            for other in range(j + 1, GROUP):
                scale = tuple(part[r : r + 1] * inv for part in spread[other][t])
                spread[other] = [
                    less_product(tile, c, scale) for tile, c in zip(spread[other], column)
                ]
                spread[other][t] = tuple(
                    jnp.where(this, s, part) for s, part in zip(scale, spread[other][t])
                )
    return tiles


def solve_kernel(arr_ref, noise_ref, place_ref, out_ref, *, sources):
    def total(j):
        acc = arr_ref[0, j].astype(jnp.float32)
        for s in range(1, sources):
            acc = acc + arr_ref[s, j].astype(jnp.float32)
        return acc

    s0, s1 = total(0), total(1)
    row = lax.broadcasted_iota(jnp.int32, (LAYERS, 128), 0)
    lane = lax.broadcasted_iota(jnp.int32, (LAYERS, 128), 1)
    upper = lane >= LAYERS
    col = jnp.where(upper, lane - LAYERS, lane)
    q = jnp.where(upper, s1[:, 256:], pltpu.roll(s0[:, 256:], LAYERS, axis=1))
    qt = jnp.concatenate([q, jnp.zeros_like(q)], axis=0).T
    qt = jnp.where(upper, pltpu.roll(qt[LAYERS:], LAYERS, axis=1), qt[:LAYERS])
    ar = jnp.where(row >= col, q, qt) + jnp.where(row == col, noise_ref[...], 0.0)
    ai = jnp.where(col > row, q, jnp.where(col < row, -qt, 0.0))
    base = jnp.where(upper, LAYERS, 0)
    tiles = [(ar[i : i + TILE], ai[i : i + TILE]) for i in range(0, LAYERS, TILE)]
    tiles = inverse_tiles(tiles, col[:TILE], base[:TILE])
    ar = jnp.concatenate([tile[0] for tile in tiles], axis=0)
    ai = jnp.concatenate([tile[1] for tile in tiles], axis=0)
    z = jnp.concatenate([s0[:, : 2 * RES], s1[:, : 2 * RES]], axis=0)
    rows = []
    for half in (~upper, upper):
        left = jnp.concatenate([jnp.where(half, ar, 0.0), jnp.where(half, ai, 0.0)], axis=0)
        r = jnp.dot(left, z, precision=lax.Precision.HIGHEST, preferred_element_type=jnp.float32)
        rows.append(r[:LAYERS] - rotated(r[LAYERS:], RES))
    x = jnp.concatenate(rows, axis=0).astype(jnp.bfloat16)
    out_ref[...] = jnp.dot(place_ref[...], x, preferred_element_type=jnp.float32).astype(jnp.bfloat16)


def solve_and_route(arrived, noise, place):
    return pl.pallas_call(
        functools.partial(solve_kernel, sources=arrived.shape[0]),
        in_specs=[pl.BlockSpec(memory_space=pltpu.VMEM)] * 3,
        out_specs=pl.BlockSpec(memory_space=pltpu.VMEM),
        out_shape=jax.ShapeDtypeStruct((place.shape[0], 2 * RES), jnp.bfloat16),
        name="solve_and_route",
    )(pltpu.with_memory_space_constraint(arrived, pltpu.VMEM), noise, place)


def body(channel, received, keep_list, alloc, noise_var, owner):
    panel_count = lax.axis_size("panel")
    prb_count = lax.axis_size("prb")
    prb_local = channel.shape[1]
    prb_own = prb_local // panel_count
    pats = jnp.sum(jnp.where(keep_list < NBLK, 1 << keep_list, 0), axis=-1).astype(jnp.int32)
    sums = panel_sums(pats, channel, received)
    parts = sums.reshape(panel_count, prb_own, LAYERS, PACK)
    arrived = lax.all_to_all(parts, "panel", split_axis=0, concat_axis=0, tiled=True)

    first_prb = lax.axis_index("prb") * prb_local + lax.axis_index("panel") * prb_own
    alloc_rows = lax.dynamic_slice_in_dim(alloc, first_prb, prb_own, 0)
    owner_rows = lax.dynamic_slice_in_dim(owner, first_prb, prb_own, 0).reshape(-1)
    users = jnp.arange(noise_var.shape[0], dtype=jnp.int32)
    matches = alloc_rows[:, :, None] == users[None, None, :]
    noise = jnp.sum(jnp.where(matches, noise_var[None, None, :], jnp.float32(0.0)), axis=-1)
    devices = panel_count * prb_count
    capacity = 2
    total = owner_rows.shape[0]
    same = owner_rows[:, None] == owner_rows[None, :]
    before = jnp.arange(total)[:, None] < jnp.arange(total)[None, :]
    slots = jnp.sum(jnp.where(same & before, 1, 0), axis=0)
    target = owner_rows * capacity + slots
    place = (jnp.arange(devices * capacity)[:, None] == target[None, :]).astype(jnp.bfloat16)

    outgoing = solve_and_route(arrived, noise.reshape(1, -1), place)
    shaped = outgoing.reshape(devices, capacity, 2 * RES)
    final = lax.all_to_all(shaped, ("panel", "prb"), split_axis=0, concat_axis=0, tiled=True)
    return final.reshape(-1, 2 * RES).astype(jnp.float32)


def solution(mesh):
    placed = (
        P("panel", "prb", None, None),
        P("panel", "prb", None, None),
        P("panel", "prb", None),
        P(),
        P(),
        P(),
    )
    return jax.shard_map(
        body, mesh=mesh, in_specs=placed, out_specs=P(("panel", "prb"), None), check_vma=False
    )
```

```python
import functools

import jax
import jax.numpy as jnp
import ml_dtypes
import numpy as np
from jax import lax
from jax.experimental import pallas as pl
from jax.experimental.pallas import tpu as pltpu
from jax.sharding import PartitionSpec as P

EDGE = 8
ANT = EDGE * EDGE
NBLK = 4
LAYERS = 64
RES = 144
PACK = 384


def projector_tables():
    pos = np.arange(ANT)
    first, second = pos // EDGE, pos % EDGE
    phase = (first[:, None] * first[None, :] + second[:, None] * second[None, :]) % EDGE
    cos8 = np.array([1.0, np.sqrt(0.5), 0.0, -np.sqrt(0.5), -1.0, -np.sqrt(0.5), 0.0, np.sqrt(0.5)])
    sin8 = np.array([0.0, np.sqrt(0.5), 1.0, np.sqrt(0.5), 0.0, -np.sqrt(0.5), -1.0, -np.sqrt(0.5)])
    real = (cos8[phase] / EDGE).astype(ml_dtypes.bfloat16).astype(np.float64)
    imag = (-sin8[phase] / EDGE).astype(ml_dtypes.bfloat16).astype(np.float64)
    beams = real + 1j * imag
    table = np.zeros((2, 1 << NBLK, ANT, 4 * ANT), np.float64)
    rows = ANT // NBLK
    for pattern in range(1 << NBLK):
        keep = np.array([(pattern >> (q // rows)) & 1 for q in range(ANT)], np.float64)
        proj = np.conj(beams.T) @ (keep[:, None] * beams)
        for half in range(2):
            table[half, pattern, :, half * ANT : (half + 1) * ANT] = proj.real
            table[half, pattern, :, (2 + half) * ANT : (3 + half) * ANT] = proj.imag
    return table.astype(ml_dtypes.bfloat16)


TABLE = projector_tables()


def rotated(m, width):
    return jnp.concatenate([m[:, width:], -m[:, :width]], axis=1)


def sums_kernel(
    pats_ref, table_hbm, ch_hbm, rx_hbm, out_hbm, table_ref, ch_buf, rx_buf, out_buf, table_sem,
    in_sems, out_sems, *, panels, pieces, prbs,
):
    def incoming(i):
        rows = pl.ds(i * prbs, prbs)
        return (
            pltpu.make_async_copy(ch_hbm.at[:, rows], ch_buf.at[:, rows], in_sems.at[0, i]),
            pltpu.make_async_copy(rx_hbm.at[:, rows], rx_buf.at[:, rows], in_sems.at[1, i]),
        )

    def leaving(i):
        rows = pl.ds(i * prbs, prbs)
        return pltpu.make_async_copy(out_buf.at[rows], out_hbm.at[rows], out_sems.at[i])

    table_copy = pltpu.make_async_copy(table_hbm, table_ref, table_sem)
    table_copy.start()
    for copy in incoming(0):
        copy.start()
    table_copy.wait()
    for copy in incoming(1):
        copy.start()
    row = lax.broadcasted_iota(jnp.int32, (LAYERS, 128), 0)
    lane = lax.broadcasted_iota(jnp.int32, (LAYERS, 128), 1)

    def piece(i, carry):
        for copy in incoming(i):
            copy.wait()

        @pl.when(i + 2 < pieces)
        def _():
            for copy in incoming(i + 2):
                copy.start()

        for j in range(prbs):
            local = i * prbs + j
            pieces_t = []
            for n in range(0, panels, 2):
                pair = ch_buf[n : n + 2, local].reshape(2 * ANT, 2 * LAYERS)
                weights = jnp.concatenate(
                    [
                        table_ref[0, pats_ref[n, local]],
                        table_ref[1, pats_ref[n + 1, local]],
                    ],
                    axis=0,
                )
                ab = jnp.dot(pair.T, weights, preferred_element_type=jnp.float32)
                a, b = ab[:, : 2 * ANT], ab[:, 2 * ANT :]
                pieces_t.append(
                    jnp.concatenate(
                        [a[:LAYERS] + b[LAYERS:], a[LAYERS:] - b[:LAYERS]], axis=0
                    ).astype(jnp.bfloat16)
                )
            left = jnp.concatenate(pieces_t, axis=1)
            ch = ch_buf[:, local].reshape(panels * ANT, 2 * LAYERS)
            rx = rx_buf[:, local].reshape(panels * ANT, 2 * RES)
            head = jnp.dot(left, rx[:, :256], preferred_element_type=jnp.float32)
            rest = jnp.dot(
                left, jnp.concatenate([ch, rx[:, 256:]], axis=1), preferred_element_type=jnp.float32
            )
            my = jnp.concatenate([head, rest[:, 128:]], axis=1)
            mh = rest[:, :128]
            z = my[:LAYERS] + rotated(my[LAYERS:], RES)
            g = mh[:LAYERS] + rotated(mh[LAYERS:], LAYERS)
            swapped = pltpu.roll(g, LAYERS, axis=1)
            packed = jnp.where(row >= lane - LAYERS, swapped, g)
            tail = jnp.concatenate([z[:, 256:], jnp.zeros((LAYERS, 96), jnp.float32)], axis=1)
            out_buf[local, :, :256] = z[:, :256].astype(out_buf.dtype)
            out_buf[local, :, 256:] = jnp.where(lane >= LAYERS, packed, tail).astype(out_buf.dtype)
        leaving(i).start()
        return carry

    lax.fori_loop(0, pieces, piece, 0)
    for i in range(pieces):
        leaving(i).wait()


def panel_sums(pats, channel, received, prbs=8):
    panels, prb_local = channel.shape[:2]
    pieces = prb_local // prbs
    kernel = functools.partial(sums_kernel, panels=panels, pieces=pieces, prbs=prbs)
    return pl.pallas_call(
        kernel,
        grid_spec=pltpu.PrefetchScalarGridSpec(
            num_scalar_prefetch=1,
            grid=(1,),
            in_specs=[pl.BlockSpec(memory_space=pl.ANY)] * 3,
            out_specs=pl.BlockSpec(memory_space=pl.ANY),
            scratch_shapes=[
                pltpu.VMEM(TABLE.shape, jnp.bfloat16),
                pltpu.VMEM((panels, prb_local, ANT, 2 * LAYERS), jnp.bfloat16),
                pltpu.VMEM((panels, prb_local, ANT, 2 * RES), jnp.bfloat16),
                pltpu.VMEM((prb_local, LAYERS, PACK), jnp.bfloat16),
                pltpu.SemaphoreType.DMA(()),
                pltpu.SemaphoreType.DMA((2, pieces)),
                pltpu.SemaphoreType.DMA((pieces,)),
            ],
        ),
        out_shape=jax.ShapeDtypeStruct((prb_local, LAYERS, PACK), jnp.bfloat16),
        compiler_params=pltpu.CompilerParams(dimension_semantics=("arbitrary",)),
        name="panel_sums",
    )(pats, jnp.asarray(TABLE), channel, received)


TILE = 8
GROUP = 8


def less_product(acc, left, right):
    return (
        acc[0] - (left[0] * right[0] - left[1] * right[1]),
        acc[1] - (left[0] * right[1] + left[1] * right[0]),
    )


def inverse_tiles(tiles, col, base):
    count = len(tiles) * TILE
    row = lax.broadcasted_iota(jnp.int32, col.shape, 0)
    for k in range(0, count, GROUP):
        spread = []
        for j in range(GROUP):
            idx = base + (k + j)
            spread.append(
                [
                    tuple(
                        jnp.take_along_axis(part, idx, axis=1, mode="promise_in_bounds")
                        for part in tile
                    )
                    for tile in tiles
                ]
            )
        for j in range(GROUP):
            at = k + j
            t, r = at // TILE, at % TILE
            here = col == at
            this = row == r
            column = spread[j]
            inv = 1.0 / column[t][0][r : r + 1]
            pivot = (
                jnp.where(here[:1], inv, tiles[t][0][r : r + 1] * inv),
                jnp.where(here[:1], 0.0, tiles[t][1][r : r + 1] * inv),
            )
            tiles = [
                less_product(tuple(jnp.where(here, 0.0, part) for part in tile), c, pivot)
                for tile, c in zip(tiles, column)
            ]
            tiles[t] = tuple(jnp.where(this, p, part) for p, part in zip(pivot, tiles[t]))
            for other in range(j + 1, GROUP):
                scale = tuple(part[r : r + 1] * inv for part in spread[other][t])
                spread[other] = [
                    less_product(tile, c, scale) for tile, c in zip(spread[other], column)
                ]
                spread[other][t] = tuple(
                    jnp.where(this, s, part) for s, part in zip(scale, spread[other][t])
                )
    return tiles


def solve_kernel(arr_ref, noise_ref, place_ref, out_ref, *, sources):
    def total(j):
        acc = arr_ref[0, j].astype(jnp.float32)
        for s in range(1, sources):
            acc = acc + arr_ref[s, j].astype(jnp.float32)
        return acc

    s0, s1 = total(0), total(1)
    row = lax.broadcasted_iota(jnp.int32, (LAYERS, 128), 0)
    lane = lax.broadcasted_iota(jnp.int32, (LAYERS, 128), 1)
    upper = lane >= LAYERS
    col = jnp.where(upper, lane - LAYERS, lane)
    q = jnp.where(upper, s1[:, 256:], pltpu.roll(s0[:, 256:], LAYERS, axis=1))
    qt = jnp.concatenate([q, jnp.zeros_like(q)], axis=0).T
    qt = jnp.where(upper, pltpu.roll(qt[LAYERS:], LAYERS, axis=1), qt[:LAYERS])
    ar = jnp.where(row >= col, q, qt) + jnp.where(row == col, noise_ref[...], 0.0)
    ai = jnp.where(col > row, q, jnp.where(col < row, -qt, 0.0))
    base = jnp.where(upper, LAYERS, 0)
    tiles = [(ar[i : i + TILE], ai[i : i + TILE]) for i in range(0, LAYERS, TILE)]
    tiles = inverse_tiles(tiles, col[:TILE], base[:TILE])
    ar = jnp.concatenate([tile[0] for tile in tiles], axis=0)
    ai = jnp.concatenate([tile[1] for tile in tiles], axis=0)
    z = jnp.concatenate([s0[:, : 2 * RES], s1[:, : 2 * RES]], axis=0)
    rows = []
    for half in (~upper, upper):
        left = jnp.concatenate([jnp.where(half, ar, 0.0), jnp.where(half, ai, 0.0)], axis=0)
        r = jnp.dot(left, z, precision=lax.Precision.HIGHEST, preferred_element_type=jnp.float32)
        rows.append(r[:LAYERS] - rotated(r[LAYERS:], RES))
    x = jnp.concatenate(rows, axis=0).astype(jnp.bfloat16)
    out_ref[...] = jnp.dot(place_ref[...], x, preferred_element_type=jnp.float32).astype(jnp.bfloat16)


def solve_and_route(arrived, noise, place):
    held = [pltpu.with_memory_space_constraint(v, pltpu.VMEM) for v in (arrived, noise, place)]
    return pl.pallas_call(
        functools.partial(solve_kernel, sources=arrived.shape[0]),
        in_specs=[pl.BlockSpec(memory_space=pltpu.VMEM)] * 3,
        out_specs=pl.BlockSpec(memory_space=pltpu.VMEM),
        out_shape=pltpu.VMEM((place.shape[0], 2 * RES), jnp.bfloat16),
        name="solve_and_route",
    )(*held)


def body(channel, received, keep_list, alloc, noise_var, owner):
    panel_count = lax.axis_size("panel")
    prb_count = lax.axis_size("prb")
    prb_local = channel.shape[1]
    prb_own = prb_local // panel_count
    pats = jnp.sum(jnp.where(keep_list < NBLK, 1 << keep_list, 0), axis=-1).astype(jnp.int32)
    sums = panel_sums(pats, channel, received)
    parts = sums.reshape(panel_count, prb_own, LAYERS, PACK)
    arrived = lax.all_to_all(parts, "panel", split_axis=0, concat_axis=0, tiled=True)

    first_prb = lax.axis_index("prb") * prb_local + lax.axis_index("panel") * prb_own
    alloc_rows = lax.dynamic_slice_in_dim(alloc, first_prb, prb_own, 0)
    owner_rows = lax.dynamic_slice_in_dim(owner, first_prb, prb_own, 0).reshape(-1)
    users = jnp.arange(noise_var.shape[0], dtype=jnp.int32)
    matches = alloc_rows[:, :, None] == users[None, None, :]
    noise = jnp.sum(jnp.where(matches, noise_var[None, None, :], jnp.float32(0.0)), axis=-1)
    devices = panel_count * prb_count
    capacity = 2
    total = owner_rows.shape[0]
    same = owner_rows[:, None] == owner_rows[None, :]
    before = jnp.arange(total)[:, None] < jnp.arange(total)[None, :]
    slots = jnp.sum(jnp.where(same & before, 1, 0), axis=0)
    target = owner_rows * capacity + slots
    place = (jnp.arange(devices * capacity)[:, None] == target[None, :]).astype(jnp.bfloat16)

    outgoing = solve_and_route(arrived, noise.reshape(1, -1), place)
    shaped = outgoing.reshape(devices, capacity, 2 * RES)
    final = lax.all_to_all(shaped, ("panel", "prb"), split_axis=0, concat_axis=0, tiled=True)
    return final.reshape(-1, 2 * RES).astype(jnp.float32)


def solution(mesh):
    placed = (
        P("panel", "prb", None, None),
        P("panel", "prb", None, None),
        P("panel", "prb", None),
        P(),
        P(),
        P(),
    )
    return jax.shard_map(
        body, mesh=mesh, in_specs=placed, out_specs=P(("panel", "prb"), None), check_vma=False
    )
```
